32 devices in a mesh: rep: 8 (over y, x, core), ep: 4 (over z).
Axes of the slice: x: 2, y: 2, z: 4, core: 2. Of those that a mesh axis runs over, the one named last changes fastest.
Arguments:
- tokens: bfloat16 [2, 512, 4096], P(None, 'ep', 'rep'), may hold values from -6 to 6
- expert_ids: int32 [2, 512, 2], P(None, 'ep'), may hold values from 0 to 3, all different within a row; in each aligned block of 128 rows (0 to 127, 128 to 255, ..., all dimensions but the last counted through in order) at most 96 rows name the same one
- router_weight: bfloat16 [4096, 4], P('rep'), may hold values from -0.09375 to 0.09375
- w_gate: bfloat16 [4, 4096, 8192], P('ep', None, 'rep'), may hold values from -0.09375 to 0.09375
- w_up: bfloat16 [4, 4096, 8192], P('ep', None, 'rep'), may hold values from -0.09375 to 0.09375
- w_down: bfloat16 [4, 8192, 4096], P('ep', 'rep'), may hold values from -0.0625 to 0.0625
- cotangent: bfloat16 [2, 512, 4096], P(None, 'ep', 'rep'), may hold values from -6 to 6
Outputs:
- mixed: bfloat16 [2, 512, 4096], P(None, 'ep', 'rep')
- token_grad: bfloat16 [2, 512, 4096], P(None, 'ep', 'rep')
- gate_grad: bfloat16 [4, 4096, 8192], P('ep', None, 'rep')
- up_grad: bfloat16 [4, 4096, 8192], P('ep', None, 'rep')
- down_grad: bfloat16 [4, 8192, 4096], P('ep', 'rep')
- router_grad: float32 [4096, 4], P('rep')
The draws below stay inside these ranges and needn't reach their ends.
Inputs may be any that keep to these rules, and one draw needn't show every extreme that they name: `expert_ids`: each row names 2 different experts. Among the 128 rows of one index of ep in one microbatch no expert is named by more than 96 rows, and in every draw some expert is named by exactly 96 of them.
All inputs are finite; a program needn't handle non-finite values.
Results may differ from the reference program's by a relative error of at most 0.025.
Values may be sent and summed in bfloat16 or wider, within the bound.
A program may use at most 192 MiB of HBM per device.

```python
import math
import jax
import jax.numpy as jnp
import numpy as np
from jax import lax

D = 4096
FF = 8192
EXPERTS = 4
TOP = 2
TOK_DEV = 128
MICRO = 2
CAP = 96
TOKENS = 512
N_REP = 8
N_EP = 4


def shard_levels(own_key, shape, shards, low, largest):
    factor_of, own = 1.0, jax.random.fold_in(own_key, 6)
    for axis_at, blocks in shards:
        draws = jnp.exp(jax.random.uniform(jax.random.fold_in(own, axis_at), (blocks,), jnp.float32, low / len(shards), largest / len(shards)))
        factor_of = factor_of * jnp.repeat(draws, shape[axis_at] // blocks).reshape([-1 if axis == axis_at else 1 for axis in range(len(shape))])
    return factor_of


def shared_out(rng, own, number, rows, number_of, top, reach, skew):
    sequence = jax.random.permutation(rng, number_of)
    packed, ordinary = shares(number_of, rows * top, reach, skew, True), shares(number_of, rows * top, reach, skew, False)
    places = jnp.arange(number_of)

    def named(tallies, turn):
        used = int((tallies > 0).sum())
        fixed = max(1, used // 4)
        passed = fixed + (places - fixed + turn * (used - fixed)) % max(1, number_of - fixed)
        return jnp.zeros((number_of,), jnp.int32).at[sequence[jnp.where(places < fixed, places, passed)]].set(jnp.asarray(tallies, jnp.int32))

    tallies = jnp.where(number % 4 == 0, named(packed, number // 4), named(ordinary, number - number // 4 - 1))
    mixed = jax.random.permutation(jax.random.fold_in(own, 3), number_of)
    donor, sink = mixed[0:number_of // 2 * 2:2], mixed[1:number_of // 2 * 2:2]
    room = jnp.minimum(tallies[donor] - 1, reach - tallies[sink]) // 2
    room = jnp.where((donor == sequence[0]) | (sink == sequence[0]) | (tallies[sink] == 0), 0, jnp.maximum(room, 0))
    passed = jax.random.randint(jax.random.fold_in(own, 4), (number_of // 2,), 0, 1 << 20) % (room + 1)
    tallies = tallies.at[donor].add(-passed).at[sink].add(passed)
    members = jnp.searchsorted(jnp.cumsum(tallies), jnp.arange(rows * top), side="right").astype(jnp.int32)
    listing = members.reshape(top, rows).T
    listing = listing[jax.random.permutation(jax.random.fold_in(own, 1), rows)]
    turn = jax.random.randint(jax.random.fold_in(own, 2), (rows, 1), 0, top)
    return jnp.take_along_axis(listing, (jnp.arange(top)[None, :] + turn) % top, axis=1)


def shares(number_of, total, reach, skew, full):
    weights = [(1 << 20) // math.isqrt(standing ** skew) + 1 for standing in range(1, number_of + 1)]
    largest = reach if full else min(reach, max(-(-total // number_of), total * weights[0] // sum(weights)))
    least = 1 if total - largest >= number_of - 1 else 0
    holding, rest = [largest] + [least] * (number_of - 1), total - largest - least * (number_of - 1)
    while rest > 0:
        candidates = [i for i in range(1, number_of) if holding[i] < largest] or [i for i in range(1, number_of) if holding[i] < reach]
        whole, budget = sum([weights[i] for i in candidates]), rest
        for i in candidates:
            addition = min(reach - holding[i], max(1, budget * weights[i] // whole), rest)
            holding[i] = holding[i] + addition
            rest = rest - addition
    return np.array(holding)


def normal_values(rng, dims, scale, bound, shards=(), kind=jnp.bfloat16):
    entries = jax.random.normal(rng, dims, jnp.float32) * scale
    if len(shards) > 0:
        entries = shard_levels(rng, dims, shards, -0.22, 0.18) * entries
    return jnp.clip(entries, min=-bound, max=bound).astype(kind)


def setup_inputs(seed: int = 0) -> dict:
    splits = jax.random.split(jax.random.key(seed), 8)
    tokens = normal_values(splits[0], (MICRO, TOKENS, D), 1.0, 6.0, ((1, 4), (2, 8)))
    expert_ids_keys = jax.random.split(jax.random.fold_in(splits[1], 1), MICRO * TOKENS // TOK_DEV)
    expert_ids_turns = jax.random.permutation(jax.random.fold_in(splits[1], 3), MICRO * TOKENS // TOK_DEV)
    expert_ids = jax.vmap(lambda own, number: shared_out(jax.random.fold_in(splits[1], 2), own, number, TOK_DEV, EXPERTS, TOP, CAP, 2))(expert_ids_keys, expert_ids_turns).reshape((MICRO, TOKENS, TOP))
    router_weight = normal_values(splits[2], (D, EXPERTS), D ** -0.5, 0.09375, ((0, 8),))
    w_gate = normal_values(splits[3], (EXPERTS, D, FF), D ** -0.5, 0.09375, ((0, 4), (2, 8)))
    w_up = normal_values(splits[4], (EXPERTS, D, FF), D ** -0.5, 0.09375, ((0, 4), (2, 8)))
    w_down = normal_values(splits[5], (EXPERTS, FF, D), FF ** -0.5, 0.0625, ((0, 4), (1, 8)))
    cotangent = normal_values(splits[6], (MICRO, TOKENS, D), 1.0, 6.0, ((1, 4), (2, 8)))
    return dict(tokens=tokens, expert_ids=expert_ids, router_weight=router_weight, w_gate=w_gate, w_up=w_up, w_down=w_down, cotangent=cotangent)


def positions(route_ids):
    hits = route_ids[:, :, None] == jnp.arange(EXPERTS, dtype=jnp.int32)[None, None, :]
    per_token = jnp.sum(hits.astype(jnp.int32), axis=1)
    before = jnp.cumsum(per_token, axis=0) - per_token
    return jnp.sum(jnp.where(hits, before[:, None, :], 0), axis=2).astype(jnp.int32)


def widen(value):
    return lax.optimization_barrier(value.astype(jnp.bfloat16)).astype(jnp.float32)


def expert_forward(rows_in, gate_w, up_w):
    pre_gate = jnp.dot(rows_in, gate_w, preferred_element_type=jnp.float32)
    pre_up = jnp.dot(rows_in, up_w, preferred_element_type=jnp.float32)
    hidden = (jax.nn.silu(pre_gate) * pre_up).astype(jnp.bfloat16)
    return pre_gate, pre_up, hidden


def grouped_down(hidden, down_w):
    group = FF // N_REP
    slots = hidden.shape[0]
    parts_h = hidden.reshape(slots, N_REP, group).transpose(1, 0, 2)
    parts_w = down_w.reshape(N_REP, group, D)

    def add(total, pair):
        return total + widen(jnp.dot(pair[0], pair[1], preferred_element_type=jnp.float32)), None

    total, _ = lax.scan(add, jnp.zeros((slots, D), jnp.float32), (parts_h, parts_w))
    return total.astype(jnp.bfloat16)


def grouped_in(gate_part, up_part, gate_w, up_w):
    group = FF // N_REP
    slots = gate_part.shape[0]
    parts_g = gate_part.reshape(slots, N_REP, group).transpose(1, 0, 2)
    parts_u = up_part.reshape(slots, N_REP, group).transpose(1, 0, 2)
    weights_g = gate_w.reshape(D, N_REP, group).transpose(1, 0, 2)
    weights_u = up_w.reshape(D, N_REP, group).transpose(1, 0, 2)

    def add(total, items):
        term = jnp.dot(items[0], items[2].T, preferred_element_type=jnp.float32)
        term = term + jnp.dot(items[1], items[3].T, preferred_element_type=jnp.float32)
        return total + widen(term), None

    total, _ = lax.scan(add, jnp.zeros((slots, D), jnp.float32), (parts_g, parts_u, weights_g, weights_u))
    return total.astype(jnp.bfloat16)


def reference(tokens, expert_ids, router_weight, w_gate, w_up, w_down, cotangent):
    slot_count = N_EP * CAP
    source = jnp.arange(TOKENS, dtype=jnp.int32) // TOK_DEV
    plans = []
    inputs = []
    for step in range(MICRO):
        route_ids = expert_ids[step].astype(jnp.int32)
        places = jax.vmap(positions)(route_ids.reshape(N_EP, TOK_DEV, TOP)).reshape(TOKENS, TOP)
        row_ids = (source[:, None] * CAP + places).astype(jnp.int32)
        values = jnp.broadcast_to(tokens[step][:, None, :], (TOKENS, TOP, D))
        inputs.append(jnp.zeros((EXPERTS, slot_count, D), jnp.bfloat16).at[route_ids, row_ids].set(values))
        plans.append((route_ids, row_ids))
    expert_in = jnp.stack(inputs, axis=1)

    def forward_one(items):
        rows_all, gate_w, up_w, down_w = items
        outs = []
        for step in range(MICRO):
            pre_gate, pre_up, hidden = expert_forward(rows_all[step], gate_w, up_w)
            outs.append(grouped_down(hidden, down_w))
        return jnp.stack(outs)

    expert_out = lax.map(forward_one, (expert_in, w_gate, w_up, w_down))
    mixed = []
    cots = []
    logit_grads = []
    router_grad = jnp.zeros((D, EXPERTS), jnp.float32)
    for step in range(MICRO):
        route_ids, row_ids = plans[step]
        logits = jnp.dot(tokens[step], router_weight, preferred_element_type=jnp.float32)
        hits = route_ids[:, :, None] == jnp.arange(EXPERTS, dtype=jnp.int32)[None, None, :]
        chosen = jnp.sum(jnp.where(hits, logits[:, None, :], 0.0), axis=2)
        spread = chosen[:, 0] - chosen[:, 1]
        gates = jnp.stack([jax.nn.sigmoid(spread), jax.nn.sigmoid(-spread)], axis=1)
        pairs = expert_out[:, step][route_ids, row_ids].astype(jnp.float32)
        mixed.append((gates[:, 0, None] * pairs[:, 0] + gates[:, 1, None] * pairs[:, 1]).astype(jnp.bfloat16))
        cot = cotangent[step].astype(jnp.float32)
        gate_dots = jnp.sum(cot[:, None, :] * pairs, axis=2)
        delta = (gate_dots[:, 0] - gate_dots[:, 1]) * gates[:, 0] * gates[:, 1]
        logit_grad = delta[:, None] * (hits[:, 0].astype(jnp.float32) - hits[:, 1].astype(jnp.float32))
        logit_grads.append(logit_grad)
        router_grad = router_grad + jnp.dot(tokens[step].astype(jnp.float32).T, logit_grad, precision=lax.Precision.HIGHEST)
        cot_pairs = (gates[:, :, None] * cot[:, None, :]).astype(jnp.bfloat16)
        cots.append(jnp.zeros((EXPERTS, slot_count, D), jnp.bfloat16).at[route_ids, row_ids].set(cot_pairs))
    expert_cot = jnp.stack(cots, axis=1)

    def backward_one(items):
        rows_all, cots_all, gate_w, up_w, down_w = items
        gate_acc = jnp.zeros((D, FF), jnp.float32)
        up_acc = jnp.zeros((D, FF), jnp.float32)
        down_acc = jnp.zeros((FF, D), jnp.float32)
        grads_in = []
        for step in range(MICRO):
            rows_in = rows_all[step]
            cot_rows = cots_all[step]
            pre_gate, pre_up, hidden = expert_forward(rows_in, gate_w, up_w)
            hidden_grad = jnp.dot(cot_rows, down_w.T, preferred_element_type=jnp.float32)
            gate_sig = jax.nn.sigmoid(pre_gate)
            gate_act = pre_gate * gate_sig
            pre_gate_grad = (hidden_grad * pre_up * (gate_sig * (1.0 + pre_gate * (1.0 - gate_sig)))).astype(jnp.bfloat16)
            pre_up_grad = (hidden_grad * gate_act).astype(jnp.bfloat16)
            down_acc = down_acc + jnp.dot(hidden.T, cot_rows, preferred_element_type=jnp.float32)
            gate_acc = gate_acc + jnp.dot(rows_in.T, pre_gate_grad, preferred_element_type=jnp.float32)
            up_acc = up_acc + jnp.dot(rows_in.T, pre_up_grad, preferred_element_type=jnp.float32)
            grads_in.append(grouped_in(pre_gate_grad, pre_up_grad, gate_w, up_w))
        return gate_acc.astype(jnp.bfloat16), up_acc.astype(jnp.bfloat16), down_acc.astype(jnp.bfloat16), jnp.stack(grads_in)

    gate_grad, up_grad, down_grad, expert_in_grad = lax.map(backward_one, (expert_in, expert_cot, w_gate, w_up, w_down))
    token_grad = []
    for step in range(MICRO):
        route_ids, row_ids = plans[step]
        pairs = expert_in_grad[:, step][route_ids, row_ids].astype(jnp.float32)
        router_in = jnp.dot(logit_grads[step], router_weight.astype(jnp.float32).T, precision=lax.Precision.HIGHEST)
        token_grad.append((pairs[:, 0] + pairs[:, 1] + router_in).astype(jnp.bfloat16))
    return jnp.stack(mixed), jnp.stack(token_grad), gate_grad, up_grad, down_grad, router_grad
```

```python
import functools

import jax
import jax.numpy as jnp
from jax import lax
from jax.experimental import pallas as pl
from jax.experimental.pallas import tpu as pltpu
from jax.sharding import Mesh, PartitionSpec as P

MESH = pl.DeviceIdType.MESH
SQUARE = 4
TOP = 2
CORES = 2
VMEM_BYTES = 67043328
F32 = jnp.float32
BF16 = jnp.bfloat16


def contract(left, right, left_dim, right_dim):
    return lax.dot_general(
        left, right, (((left_dim,), (right_dim,)), ((), ())), preferred_element_type=F32
    )


def swap(value, cores):
    return lax.ppermute(value, "core", [(i, cores - 1 - i) for i in range(cores)])


def gather_features(rows, core, earlier=None):
    mine = lax.all_gather(rows, "chip", axis=0, tiled=False)
    if earlier is not None:
        mine = after(mine, earlier)
    other = swap(mine, CORES)
    pieces = []
    for chip in range(mine.shape[0]):
        pieces.append(jnp.where(core == 0, mine[chip], other[chip]))
        pieces.append(jnp.where(core == 0, other[chip], mine[chip]))
    return jnp.concatenate(pieces, axis=1)


def core_parts(partial, core):
    chips = lax.axis_size("chip")
    width = partial.shape[1] // (chips * CORES)
    pieces = [
        lax.slice_in_dim(partial, i * width, (i + 1) * width, axis=1) for i in range(chips * CORES)
    ]
    low, high = jnp.stack(pieces[0::2]), jnp.stack(pieces[1::2])
    return jnp.where(core == 0, low, high), jnp.where(core == 0, high, low)


def pair_sum(keep, send):
    return (keep.astype(F32) + swap(send, CORES).astype(F32)).astype(BF16)


def scatter_chips(total):
    return lax.psum_scatter(total, "chip", scatter_dimension=0, tiled=False)


def exchange(rows, sign):
    count = lax.axis_size("ep")
    blocks = rows.reshape(count, -1, rows.shape[-1])
    moved = [blocks[0]]
    for d in range(1, count):
        pairs = [(i, (i + sign * d) % count) for i in range(count)]
        moved.append(lax.ppermute(blocks[d], "ep", pairs))
    return jnp.concatenate(moved, axis=0)


def after(value, earlier):
    zero = earlier[(0,) * earlier.ndim].astype(F32) * 0.0
    return value + zero.astype(value.dtype)


def route(ids, experts, capacity):
    micro, rows, _ = ids.shape
    away = lax.rem(ids - lax.axis_index("ep") + experts, experts)
    hits = ids[..., None] == jnp.arange(experts, dtype=jnp.int32)
    per_token = jnp.sum(hits.astype(F32), axis=2)
    earlier = (
        jnp.arange(rows)[:, None] > jnp.arange(rows)[None, :]
    ).astype(BF16)
    before = jnp.einsum(
        "ij,mje->mie", earlier, per_token.astype(BF16), preferred_element_type=F32
    )
    places = jnp.sum(jnp.where(hits, before[:, :, None, :], 0.0), axis=3).astype(jnp.int32)
    step = jnp.arange(micro, dtype=jnp.int32)[:, None, None]
    slots = ((away * micro + step) * capacity + places).reshape(micro * rows, TOP)
    picks = slots[:, :, None] == jnp.arange(experts * micro * capacity, dtype=jnp.int32)
    return hits.reshape(micro * rows, TOP, experts), picks[:, 0], picks[:, 1]


def shards(tokens, expert_ids, router_weight, w_gate, w_up, w_down, cotangent):
    micro, rows, width = tokens.shape
    experts = router_weight.shape[1]
    capacity = min(rows, 3 * rows * TOP // (2 * experts))
    core = lax.axis_index("core")
    gate_w, up_w, down_w = w_gate[0], w_up[0], w_down[0]
    toks = tokens.reshape(micro * rows, width)
    cots = cotangent.reshape(micro * rows, width)

    hits, pick0, pick1 = route(expert_ids, experts, capacity)
    hot0, hot1 = pick0.astype(BF16), pick1.astype(BF16)
    hot = hot0 + hot1

    moved_rows = exchange(contract(hot, toks, 0, 0).astype(BF16), 1)

    partial_logits = contract(router_weight, toks, 0, 1)
    logits = lax.psum(after(partial_logits, moved_rows), ("chip", "core")).T
    chosen = jnp.sum(jnp.where(hits, logits[:, None, :], 0.0), axis=2)
    spread = chosen[:, 0] - chosen[:, 1]
    first = jax.nn.sigmoid(spread)
    second = jax.nn.sigmoid(-spread)
    slot_gate = jnp.sum(
        jnp.where(pick0, first[:, None], 0.0) + jnp.where(pick1, second[:, None], 0.0), axis=0
    )
    sent_cots = (contract(hot, cots, 0, 0) * slot_gate[:, None]).astype(BF16)
    moved_cots = exchange(sent_cots, 1)

    expert_rows = gather_features(moved_rows, core, moved_cots)
    pre_gate = contract(expert_rows, gate_w, 1, 0)
    pre_up = contract(expert_rows, up_w, 1, 0)
    gate_sig = jax.nn.sigmoid(pre_gate)
    gate_act = pre_gate * gate_sig
    hidden = (gate_act * pre_up).astype(BF16)
    keep, send = core_parts(contract(hidden, down_w, 1, 0).astype(BF16), core)
    total = pair_sum(keep, send)
    expert_cots = after(gather_features(moved_cots, core, hidden), total)
    returned = exchange(after(scatter_chips(total), slot_gate), -1)

    hidden_grad = contract(expert_cots, down_w, 1, 1)
    gate_pre_grad = (
        hidden_grad * pre_up * (gate_sig * (1.0 + pre_gate * (1.0 - gate_sig)))
    ).astype(BF16)
    up_pre_grad = (hidden_grad * gate_act).astype(BF16)
    inputs = (contract(gate_pre_grad, gate_w, 1, 1) + contract(up_pre_grad, up_w, 1, 1)).astype(BF16)
    keep_in, send_in = core_parts(inputs, core)
    scattered_in = scatter_chips(pair_sum(keep_in, send_in))

    down_grad = contract(hidden, expert_cots, 0, 0).astype(BF16)
    gate_grad = contract(expert_rows, gate_pre_grad, 0, 0).astype(BF16)
    up_grad = contract(expert_rows, up_pre_grad, 0, 0).astype(BF16)

    first_out = contract(hot0, returned, 1, 0)
    second_out = contract(hot1, returned, 1, 0)
    mixed = (first[:, None] * first_out + second[:, None] * second_out).astype(BF16)
    cot_wide = cots.astype(F32)
    partial_dots = jnp.sum(cot_wide * (first_out - second_out), axis=1)
    partial_dots = after(partial_dots, slot_gate)
    gate_dots = lax.psum(partial_dots, ("chip", "core"))
    delta = gate_dots * first * second
    logit_grad = delta[:, None] * (hits[:, 0].astype(F32) - hits[:, 1].astype(F32))
    router_grad = lax.psum(
        lax.dot_general(
            logit_grad, toks.astype(F32), (((0,), (0,)), ((), ())), precision=lax.Precision.HIGHEST
        ),
        "ep",
    ).T
    router_in = lax.dot_general(
        logit_grad,
        router_weight.astype(F32),
        (((1,), (1,)), ((), ())),
        precision=lax.Precision.HIGHEST,
    )
    returned_grad = exchange(after(scattered_in, router_grad), -1)
    token_grad = (contract(hot, returned_grad, 1, 0) + router_in).astype(BF16)
    return (
        mixed.reshape(tokens.shape),
        token_grad.reshape(tokens.shape),
        gate_grad[None],
        up_grad[None],
        down_grad[None],
        router_grad,
    )


def dot(left, right, left_dim=1, right_dim=0):
    return lax.dot_general(
        left, right, (((left_dim,), (right_dim,)), ((), ())), preferred_element_type=F32
    )


def exact(left, right):
    return jnp.dot(left, right, precision=lax.Precision.HIGHEST, preferred_element_type=F32)


def layer_kernel(
    micro, ep_size, cap,
    part_ref, hit0_ref, hit1_ref, pick0_ref, pick1_ref, toks_ref, cots_ref, send_ref,
    wg_hbm, wu_hbm, wd_hbm,
    out_ret, in_ret, gate_out, up_out, down_out, gates_ref, logit_grad_ref, router_ref,
    x_buf, c_buf, wg, wu, wd, pg, pu, hid, gpg, upg, hg, sc_buf, stage, total, pair_in, relay_in,
    side_in, logit_buf, dots_buf, dots_z, dots_own, router_buf,
    w_sem, z_send, z_recv, z_local, ag_send, ag_recv, small_send, small_recv,
    pair_send, pair_recv, rs_send, rs_recv, back_send, back_recv, back_local, out_sem, credit,
):
    pieces, slots, width = x_buf.shape
    hidden_width = hid.shape[1]
    rows = slots // micro
    half = rows // 2
    tokens_one = pick0_ref.shape[2]
    chip, core, ep = lax.axis_index("chip"), lax.axis_index("core"), lax.axis_index("ep")
    chip_x = chip + 1 - 2 * (chip % 2)
    chip_y = (chip + 2) % SQUARE
    chip_d = SQUARE - 1 - chip
    other = 1 - core
    dev_x, dev_y, dev_pair = (chip_x, core, ep), (chip_y, core, ep), (chip, other, ep)
    me = chip * CORES + core

    def rep_peer(i):
        peer = (me + i) % pieces
        return (peer // CORES, peer % CORES, ep)

    def ep_peer(d):
        return (chip, core, (ep + d + ep_size) % ep_size)

    def remote(source, target, send, recv, device):
        return pltpu.make_async_remote_copy(
            src_ref=source, dst_ref=target, send_sem=send, recv_sem=recv,
            device_id=device, device_id_type=MESH,
        )

    def piece_of(which, kind):
        return which * CORES + kind

    barrier = pltpu.get_barrier_semaphore()
    for i in range(1, pieces):
        pl.semaphore_signal(barrier, inc=1, device_id=rep_peer(i), device_id_type=MESH)
    for d in range(1, ep_size):
        pl.semaphore_signal(barrier, inc=1, device_id=ep_peer(d), device_id_type=MESH)
    pl.semaphore_wait(barrier, pieces - 1 + ep_size - 1)

    def gather_small(source, target, base):
        copies = [
            remote(source, target.at[i], small_send.at[base + i], small_recv.at[base + i], rep_peer(i))
            for i in range(1, pieces)
        ]
        for copy in copies:
            copy.start()
        return copies

    logit_copies = gather_small(part_ref, logit_buf, 0)

    def z_copy(a, m, d):
        source = send_ref.at[m * ep_size + d] if a == 0 else sc_buf.at[m, pl.ds(d * cap, cap)]
        buf = x_buf if a == 0 else c_buf
        target = buf.at[me, pl.ds(m * rows + d * cap, cap)]
        return remote(source, target, z_send.at[a, m, d], z_recv.at[a, m, d], ep_peer(d))

    def z_home(m):
        return pltpu.make_async_copy(
            send_ref.at[m * ep_size], x_buf.at[me, pl.ds(m * rows, cap)], z_local.at[m]
        )

    for m in range(micro):
        for d in range(1, ep_size):
            z_copy(0, m, d).start()
        z_home(m).start()

    def weight_copy(i):
        if i == 0:
            return pltpu.make_async_copy(wg_hbm, wg, w_sem.at[0])
        if i == 1:
            return pltpu.make_async_copy(wu_hbm, wu, w_sem.at[1])
        return pltpu.make_async_copy(
            wd_hbm.at[:, pl.ds((i - 2) * width, width)], wd.at[i - 2], w_sem.at[i]
        )

    for i in range(2 + pieces):
        weight_copy(i).start()

    for copy in logit_copies:
        copy.wait_recv()
    logits = part_ref[...]
    for i in range(1, pieces):
        logits = logits + logit_buf[i]
    spread = jnp.sum((hit0_ref[...] - hit1_ref[...]) * logits, axis=0, keepdims=True)
    first = jax.nn.sigmoid(spread)
    second = jax.nn.sigmoid(-spread)
    row = lax.broadcasted_iota(jnp.int32, gates_ref.shape, 0)
    gates_ref[...] = jnp.where(row == 0, first, jnp.where(row == 1, second, 0.0))

    for m in range(micro):
        span = slice(m * tokens_one, (m + 1) * tokens_one)
        for d in range(ep_size):
            place = slice(d * cap, (d + 1) * cap)
            weight = jnp.sum(
                pick0_ref[m, place] * first[:, span] + pick1_ref[m, place] * second[:, span],
                axis=1, keepdims=True,
            )
            scaled = (cots_ref[m, place].astype(F32) * weight).astype(BF16)
            if d == 0:
                c_buf[me, m * rows : m * rows + cap] = scaled
            else:
                sc_buf[m, place] = scaled
        for d in range(1, ep_size):
            z_copy(1, m, d).start()

    def ag_copy(a, m, i):
        buf = x_buf if a == 0 else c_buf
        low, high = pl.ds(m * rows, half), pl.ds(m * rows + half, half)
        full = pl.ds(m * rows, rows)
        piece, span, device = [
            (me, low, dev_x), (me, high, dev_x), (me, high, dev_y), (me, low, dev_y),
            (piece_of(chip_x, core), low, dev_y), (piece_of(chip_y, core), high, dev_x),
            (me, full, dev_pair), (piece_of(chip_x, core), full, dev_pair),
            (piece_of(chip_y, core), full, dev_pair), (piece_of(chip_d, core), full, dev_pair),
        ][i]
        ref = buf.at[piece, span]
        return remote(ref, ref, ag_send.at[a, m, i], ag_recv.at[a, m, i], device)

    def ag_arrive(a, m, i):
        ag_copy(a, m, i).wait_recv()

    def ag_start(a, m):
        for d in range(1, ep_size):
            z_copy(a, m, d).wait_recv()
        if a == 0:
            z_home(m).wait()
        for i in (0, 2, 1, 3, 6):
            ag_copy(a, m, i).start()

    def ag_relay(a, m):
        ag_arrive(a, m, 0)
        ag_copy(a, m, 4).start()
        ag_arrive(a, m, 2)
        ag_copy(a, m, 5).start()
        ag_arrive(a, m, 1)
        ag_copy(a, m, 7).start()
        ag_arrive(a, m, 3)
        ag_copy(a, m, 8).start()

    def ag_diag(a, m):
        ag_arrive(a, m, 4)
        ag_arrive(a, m, 5)
        ag_copy(a, m, 9).start()

    order = (chip, chip_x, chip_y, chip_d)
    tile = 256

    def forward(m, s):
        if m == 0 and s == 0:
            weight_copy(0).wait()
            weight_copy(1).wait()
        ag_arrive(0, m, 6 + s)
        which = order[s]

        @pl.loop(0, hidden_width // tile)
        def _(n):
            cols = pl.ds(pl.multiple_of(n * tile, tile), tile)
            span = pl.ds(m * rows, rows)
            one, two = x_buf[piece_of(which, 0), span], x_buf[piece_of(which, 1), span]
            gate = dot(one, wg[piece_of(which, 0), :, cols]) + dot(two, wg[piece_of(which, 1), :, cols])
            up = dot(one, wu[piece_of(which, 0), :, cols]) + dot(two, wu[piece_of(which, 1), :, cols])
            if s == 0:
                pg[span, cols] = gate
                pu[span, cols] = up
            else:
                pg[span, cols] += gate
                pu[span, cols] += up

    strip = 32

    def activate(m):
        @pl.loop(0, rows // strip)
        def _(r):
            span = pl.ds(pl.multiple_of(m * rows + r * strip, strip), strip)
            gate, up = pg[span], pu[span]
            sig = jax.nn.sigmoid(gate)
            act = gate * sig
            hid[span] = (act * up).astype(BF16)
            pu[span] = up * (sig * (1.0 + gate * (1.0 - sig)))
            pg[span] = act

    def backward(m, s):
        ag_arrive(1, m, 6 + s)
        which = order[s]

        @pl.loop(0, hidden_width // tile)
        def _(n):
            cols = pl.ds(pl.multiple_of(n * tile, tile), tile)
            span = pl.ds(m * rows, rows)
            one, two = c_buf[piece_of(which, 0), span], c_buf[piece_of(which, 1), span]
            grad = dot(one, wd[piece_of(which, 0), cols], 1, 1) + dot(two, wd[piece_of(which, 1), cols], 1, 1)
            if s == 0:
                hg[:, cols] = grad
            else:
                hg[:, cols] += grad

    lanes = 128

    def gradients(m):
        @pl.loop(0, rows // strip)
        def _(r):
            span = pl.ds(pl.multiple_of(m * rows + r * strip, strip), strip)
            here = pl.ds(pl.multiple_of(r * strip, strip), strip)
            grad = hg[here]
            gpg[span] = (grad * pu[span]).astype(BF16)
            upg[span] = (grad * pg[span]).astype(BF16)
            both = grad * hid[span].astype(F32)
            part = both[:, :lanes]
            for i in range(1, hidden_width // lanes):
                part = part + both[:, i * lanes : (i + 1) * lanes]
            hg[here, :lanes] = part

        sums = jnp.sum(hg[:, :lanes].T, axis=0, keepdims=True)
        mark = lax.broadcasted_iota(jnp.int32, dots_own.shape, 0) == m
        if m == 0:
            dots_own[...] = jnp.where(mark, sums, 0.0)
        else:
            dots_own[...] = jnp.where(mark, sums, dots_own[...])

    def wait_down():
        for i in range(2, 2 + pieces):
            weight_copy(i).wait()

    def partial(a, m, piece, target):
        wide = width // tile

        @pl.loop(0, wide)
        def _(n):
            cols = pl.ds(pl.multiple_of(n * tile, tile), tile)
            span = pl.ds(m * rows, rows)
            if a == 0:
                value = dot(hid[span], wd[piece, :, cols])
            else:
                value = dot(gpg[span], wg[piece, cols], 1, 1) + dot(upg[span], wu[piece, cols], 1, 1)
            target[:, cols] = value.astype(BF16)

    rs_order = (chip_d, chip_x, chip_y, chip)

    def pair_copy(a, m, j):
        return remote(
            stage.at[j], pair_in.at[m, j], pair_send.at[a, m, j], pair_recv.at[a, m, j], dev_pair
        )

    low_half, high_half = pl.ds(0, half), pl.ds(half, half)

    def rs_copy(a, m, i):
        source, span, target, device = [
            (0, low_half, relay_in.at[m, 0], dev_x),
            (0, high_half, relay_in.at[m, 1], dev_y),
            (1, low_half, side_in.at[m, 0, low_half], dev_x),
            (2, high_half, side_in.at[m, 1, high_half], dev_y),
            (2, low_half, side_in.at[m, 1, low_half], dev_y),
            (1, high_half, side_in.at[m, 0, high_half], dev_x),
        ][i]
        return remote(
            total.at[m, source, span], target, rs_send.at[a, m, i], rs_recv.at[a, m, i], device
        )

    def back_copy(a, m, d):
        target = out_ret if a == 0 else in_ret
        source = total.at[m, 3, pl.ds(d * cap, cap)]
        if d == 0:
            return pltpu.make_async_copy(source, target.at[m * ep_size], back_local.at[a, m])
        return remote(
            source, target.at[m * ep_size + d], back_send.at[a, m, d], back_recv.at[a, m, d], ep_peer(-d)
        )

    def scatter_pair(a, m):
        if (a, m) != (0, 0):
            before = (a, m - 1) if m > 0 else (a - 1, micro - 1)
            for j in range(SQUARE):
                pair_copy(before[0], before[1], j).wait_send()
        if a == 1:
            pl.semaphore_wait(credit.at[m], 3)
        for j in range(SQUARE):
            partial(a, m, piece_of(rs_order[j], other), stage.at[j])
            pair_copy(a, m, j).start()
        if a == 1:
            for i in range(6):
                rs_copy(0, m, i).wait_send()
            for d in range(1, ep_size):
                back_copy(0, m, d).wait_send()
            back_copy(0, m, 0).wait()
        for j in range(SQUARE):
            partial(a, m, piece_of(rs_order[j], core), total.at[m, j])

    def add_into(m, j, start, count, others):
        @pl.loop(0, count // strip)
        def _(r):
            span = pl.ds(pl.multiple_of(start + r * strip, strip), strip)
            here = pl.ds(pl.multiple_of(r * strip, strip), strip)
            value = total[m, j, span].astype(F32)
            for ref in others:
                value = value + ref[here].astype(F32)
            total[m, j, span] = value.astype(BF16)

    def scatter_sum(a, m):
        for j in range(SQUARE):
            pair_copy(a, m, j).wait_recv()
            add_into(m, j, 0, rows, (pair_in.at[m, j],))
            if j == 0:
                rs_copy(a, m, 0).start()
                rs_copy(a, m, 1).start()
            elif j < 3:
                rs_copy(a, m, 1 + j).start()

    def scatter_relay(a, m):
        rs_copy(a, m, 0).wait_recv()
        add_into(m, 2, 0, half, (relay_in.at[m, 0],))
        rs_copy(a, m, 4).start()
        rs_copy(a, m, 1).wait_recv()
        add_into(m, 1, half, half, (relay_in.at[m, 1],))
        rs_copy(a, m, 5).start()

    def scatter_last(a, m):
        for i in (2, 3, 4, 5):
            rs_copy(a, m, i).wait_recv()
        add_into(m, 3, 0, rows, (side_in.at[m, 0], side_in.at[m, 1]))
        for d in range(1, ep_size):
            back_copy(a, m, d).start()
        back_copy(a, m, 0).start()
        if a == 0:
            for device in (dev_pair, dev_x, dev_y):
                pl.semaphore_signal(credit.at[m], inc=1, device_id=device, device_id_type=MESH)

    def out_copy(kind, piece):
        if kind == 0:
            return pltpu.make_async_copy(
                wd.at[piece], down_out.at[:, pl.ds(piece * width, width)], out_sem.at[0, piece]
            )
        if kind == 1:
            return pltpu.make_async_copy(wg.at[piece], gate_out.at[piece], out_sem.at[1, piece])
        return pltpu.make_async_copy(wu.at[piece], up_out.at[piece], out_sem.at[2, piece])

    def weight_grads(kind, start, stop):
        for piece in range(start, stop):
            if kind == 0:
                @pl.loop(0, hidden_width // tile)
                def _(n):
                    cols = pl.ds(pl.multiple_of(n * tile, tile), tile)
                    wd[piece, cols] = dot(hid[:, cols], c_buf[piece], 0, 0).astype(BF16)
            else:
                grad, keep = (gpg, wg) if kind == 1 else (upg, wu)

                @pl.loop(0, hidden_width // tile)
                def _(n):
                    cols = pl.ds(pl.multiple_of(n * tile, tile), tile)
                    keep[piece, :, cols] = dot(x_buf[piece], grad[:, cols], 0, 0).astype(BF16)
            out_copy(kind, piece).start()

    ag_start(0, 0)
    ag_start(0, 1)
    ag_relay(0, 0)
    forward(0, 0)
    ag_start(1, 0)
    ag_diag(0, 0)
    forward(0, 1)
    ag_relay(0, 1)
    forward(0, 2)
    ag_start(1, 1)
    forward(0, 3)
    ag_diag(0, 1)
    activate(0)
    ag_relay(1, 0)
    forward(1, 0)
    forward(1, 1)
    ag_diag(1, 0)
    wait_down()
    scatter_pair(0, 0)
    ag_relay(1, 1)
    scatter_sum(0, 0)
    forward(1, 2)
    forward(1, 3)
    activate(1)
    ag_diag(1, 1)
    scatter_relay(0, 0)
    scatter_pair(0, 1)
    scatter_sum(0, 1)
    for s in range(4):
        backward(0, s)
    gradients(0)
    scatter_last(0, 0)
    scatter_relay(0, 1)
    scatter_pair(1, 0)
    scatter_sum(1, 0)
    for s in range(4):
        backward(1, s)
    scatter_relay(1, 0)
    scatter_last(0, 1)
    gradients(1)
    dots_copies = gather_small(dots_own, dots_buf, pieces)
    scatter_pair(1, 1)
    scatter_sum(1, 1)
    scatter_last(1, 0)
    weight_grads(0, 0, 4)
    scatter_relay(1, 1)
    for copy in dots_copies:
        copy.wait_recv()
    dots = dots_own[...]
    for i in range(1, pieces):
        dots = dots + dots_buf[i]
    dots_z[0] = dots
    dots_back = [
        remote(dots_z.at[0], dots_z.at[d], small_send.at[2 * pieces + d], small_recv.at[2 * pieces + d], ep_peer(-d))
        for d in range(1, ep_size)
    ]
    for copy in dots_back:
        copy.start()
    weight_grads(0, 4, 8)
    scatter_last(1, 1)
    weight_grads(1, 0, 4)
    for copy in dots_back:
        copy.wait_recv()
    owner = lax.broadcasted_iota(jnp.int32, dots_own.shape, 1) // cap
    mine = jnp.where(owner == 0, dots_z[0], 0.0)
    for d in range(1, ep_size):
        mine = jnp.where(owner == d, dots_z[d], mine)
    for m in range(micro):
        span = slice(m * tokens_one, (m + 1) * tokens_one)
        zero = exact(mine, pick0_ref[m])[m : m + 1]
        one = exact(mine, pick1_ref[m])[m : m + 1]
        delta = gates_ref[1:2, span] * zero - gates_ref[0:1, span] * one
        logit_grad_ref[:, span] = delta * (hit0_ref[:, span] - hit1_ref[:, span])
    router_buf[0] = exact(logit_grad_ref[...], toks_ref[...].astype(F32))
    router_copies = [
        remote(router_buf.at[0], router_buf.at[d], small_send.at[2 * pieces + ep_size + d], small_recv.at[2 * pieces + ep_size + d], ep_peer(d))
        for d in range(1, ep_size)
    ]
    for copy in router_copies:
        copy.start()
    weight_grads(1, 4, 8)
    weight_grads(2, 0, 8)
    for copy in router_copies:
        copy.wait_recv()
    router = router_buf[0]
    for d in range(1, ep_size):
        router = router + router_buf[d]
    router_ref[...] = router

    for a in range(2):
        for m in range(micro):
            for d in range(1, ep_size):
                z_copy(a, m, d).wait_send()
                back_copy(a, m, d).wait_recv()
                if a == 1:
                    back_copy(a, m, d).wait_send()
            for i in range(10):
                ag_copy(a, m, i).wait_send()
            if a == 1:
                back_copy(a, m, 0).wait()
                for i in range(6):
                    rs_copy(a, m, i).wait_send()
    for j in range(SQUARE):
        pair_copy(1, micro - 1, j).wait_send()
    for copy in logit_copies + dots_copies + dots_back + router_copies:
        copy.wait_send()
    for kind in range(3):
        for piece in range(pieces):
            out_copy(kind, piece).wait()


def square_shards(tokens, expert_ids, router_weight, w_gate, w_up, w_down, cotangent):
    micro, rows, width = tokens.shape
    experts = router_weight.shape[1]
    capacity = min(rows, 3 * rows * TOP // (2 * experts))
    ep_size = lax.axis_size("ep")
    pieces = lax.axis_size("chip") * CORES
    count = experts * capacity
    slots = micro * count
    hidden_width = w_down.shape[1]
    sub = max(8, -(-experts // 8) * 8)
    toks = tokens.reshape(micro * rows, width)
    cots = cotangent.reshape(micro * rows, width)

    away = lax.rem(expert_ids - lax.axis_index("ep") + experts, experts)
    hits = expert_ids[..., None] == jnp.arange(experts, dtype=jnp.int32)
    per_token = jnp.sum(hits.astype(F32), axis=2)
    earlier = (jnp.arange(rows)[:, None] > jnp.arange(rows)[None, :]).astype(BF16)
    before = jnp.einsum(
        "ij,mje->mie", earlier, per_token.astype(BF16), preferred_element_type=F32
    )
    places = jnp.sum(jnp.where(hits, before[:, :, None, :], 0.0), axis=3).astype(jnp.int32)
    where_to = away * capacity + places
    picks = jnp.arange(count, dtype=jnp.int32)[None, :, None, None] == where_to[:, None]
    pick0, pick1 = picks[..., 0].astype(F32), picks[..., 1].astype(F32)
    hot0, hot1 = pick0.astype(BF16), pick1.astype(BF16)
    hot = hot0 + hot1
    send = jnp.einsum("mst,mtw->msw", hot, tokens, preferred_element_type=F32).astype(BF16)
    cot_slots = jnp.einsum("mst,mtw->msw", hot, cotangent, preferred_element_type=F32).astype(BF16)
    pad = ((0, sub - experts), (0, 0))
    part = jnp.pad(contract(router_weight, toks, 0, 1), pad)
    hit_rows = jnp.moveaxis(hits.astype(F32), -1, 0)
    hit0 = jnp.pad(hit_rows[..., 0].reshape(experts, -1), pad)
    hit1 = jnp.pad(hit_rows[..., 1].reshape(experts, -1), pad)

    vmem = pl.BlockSpec(memory_space=pltpu.VMEM)
    hbm = pl.BlockSpec(memory_space=pl.ANY)
    shape = jax.ShapeDtypeStruct
    dma = pltpu.SemaphoreType.DMA
    features = w_gate.shape[1]
    ret = shape((micro * ep_size, capacity, width), BF16)
    wide = shape((pieces, width, hidden_width), BF16)
    half = count // 2
    sizes = dict(collective_id=0, has_side_effects=True, vmem_limit_bytes=VMEM_BYTES)
    out_ret, in_ret, gate_grad, up_grad, down_grad, gates, logit_grad, router = pl.pallas_call(
        functools.partial(layer_kernel, micro, ep_size, capacity),
        out_shape=(
            ret, ret, wide, wide, shape((hidden_width, features), BF16),
            shape((sub, micro * rows), F32), shape((sub, micro * rows), F32), shape((sub, width), F32),
        ),
        in_specs=[vmem] * 7 + [hbm] * 4,
        out_specs=(hbm,) * 5 + (vmem,) * 3,
        scratch_shapes=[
            pltpu.VMEM((pieces, slots, width), BF16),
            pltpu.VMEM((pieces, slots, width), BF16),
            pltpu.VMEM((pieces, width, hidden_width), BF16),
            pltpu.VMEM((pieces, width, hidden_width), BF16),
            pltpu.VMEM((pieces, hidden_width, width), BF16),
            pltpu.VMEM((slots, hidden_width), F32),
            pltpu.VMEM((slots, hidden_width), F32),
            pltpu.VMEM((slots, hidden_width), BF16),
            pltpu.VMEM((slots, hidden_width), BF16),
            pltpu.VMEM((slots, hidden_width), BF16),
            pltpu.VMEM((count, hidden_width), F32),
            pltpu.VMEM((micro, count, width), BF16),
            pltpu.VMEM((SQUARE, count, width), BF16),
            pltpu.VMEM((micro, SQUARE, count, width), BF16),
            pltpu.VMEM((micro, SQUARE, count, width), BF16),
            pltpu.VMEM((micro, 2, half, width), BF16),
            pltpu.VMEM((micro, 2, count, width), BF16),
            pltpu.VMEM((pieces, sub, micro * rows), F32),
            pltpu.VMEM((pieces, 8, count), F32),
            pltpu.VMEM((ep_size, 8, count), F32),
            pltpu.VMEM((8, count), F32),
            pltpu.VMEM((ep_size, sub, width), F32),
            dma((2 + pieces,)),
            dma((2, micro, ep_size)),
            dma((2, micro, ep_size)),
            dma((micro,)),
            dma((2, micro, 10)),
            dma((2, micro, 10)),
            dma((2 * pieces + 2 * ep_size,)),
            dma((2 * pieces + 2 * ep_size,)),
            dma((2, micro, SQUARE)),
            dma((2, micro, SQUARE)),
            dma((2, micro, 6)),
            dma((2, micro, 6)),
            dma((2, micro, ep_size)),
            dma((2, micro, ep_size)),
            dma((2, micro)),
            dma((3, pieces)),
            pltpu.SemaphoreType.REGULAR((micro,)),
        ],
        compiler_params=pltpu.CompilerParams(**sizes),
    )(
        part, hit0, hit1, pick0, pick1, toks, cot_slots,
        send.reshape(micro * experts, capacity, width),
        w_gate.reshape(pieces, width, hidden_width),
        w_up.reshape(pieces, width, hidden_width),
        w_down[0],
    )
    returned = out_ret.reshape(micro, count, width)
    returned_in = in_ret.reshape(micro, count, width)

    def collect(chosen, values):
        return jnp.einsum("mst,msw->mtw", chosen, values, preferred_element_type=F32)

    first = gates[0].reshape(micro, rows, 1)
    second = gates[1].reshape(micro, rows, 1)
    mixed = (first * collect(hot0, returned) + second * collect(hot1, returned)).astype(BF16)
    router_in = lax.dot_general(
        logit_grad[:experts],
        router_weight.astype(F32),
        (((0,), (1,)), ((), ())),
        precision=lax.Precision.HIGHEST,
    )
    token_grad = (collect(hot, returned_in) + router_in.reshape(tokens.shape)).astype(BF16)
    return (
        mixed,
        token_grad,
        gate_grad.reshape(w_gate.shape),
        up_grad.reshape(w_up.shape),
        down_grad[None],
        router[:experts].T,
    )


def solution(mesh):
    rep, ep = mesh.shape["rep"], mesh.shape["ep"]
    inner = Mesh(mesh.devices.reshape(rep // CORES, CORES, ep), ("chip", "core", "ep"))
    reps = ("chip", "core")
    in_specs = (
        P(None, "ep", reps),
        P(None, "ep", None),
        P(reps, None),
        P("ep", None, reps),
        P("ep", None, reps),
        P("ep", reps, None),
        P(None, "ep", reps),
    )
    out_specs = (
        P(None, "ep", reps),
        P(None, "ep", reps),
        P("ep", None, reps),
        P("ep", None, reps),
        P("ep", reps, None),
        P(reps, None),
    )
    body = square_shards if rep // CORES == SQUARE else shards
    return jax.shard_map(body, mesh=inner, in_specs=in_specs, out_specs=out_specs, check_vma=False)
```

```python
import functools

import jax
import jax.numpy as jnp
from jax import lax
from jax.experimental import pallas as pl
from jax.experimental.pallas import tpu as pltpu
from jax.sharding import Mesh, PartitionSpec as P

MESH = pl.DeviceIdType.MESH
SQUARE = 4
TOP = 2
CORES = 2
VMEM_BYTES = 67043328
F32 = jnp.float32
BF16 = jnp.bfloat16


def contract(left, right, left_dim, right_dim):
    return lax.dot_general(
        left, right, (((left_dim,), (right_dim,)), ((), ())), preferred_element_type=F32
    )


def swap(value, cores):
    return lax.ppermute(value, "core", [(i, cores - 1 - i) for i in range(cores)])


def gather_features(rows, core, earlier=None):
    mine = lax.all_gather(rows, "chip", axis=0, tiled=False)
    if earlier is not None:
        mine = after(mine, earlier)
    other = swap(mine, CORES)
    pieces = []
    for chip in range(mine.shape[0]):
        pieces.append(jnp.where(core == 0, mine[chip], other[chip]))
        pieces.append(jnp.where(core == 0, other[chip], mine[chip]))
    return jnp.concatenate(pieces, axis=1)


def core_parts(partial, core):
    chips = lax.axis_size("chip")
    width = partial.shape[1] // (chips * CORES)
    pieces = [
        lax.slice_in_dim(partial, i * width, (i + 1) * width, axis=1) for i in range(chips * CORES)
    ]
    low, high = jnp.stack(pieces[0::2]), jnp.stack(pieces[1::2])
    return jnp.where(core == 0, low, high), jnp.where(core == 0, high, low)


def pair_sum(keep, send):
    return (keep.astype(F32) + swap(send, CORES).astype(F32)).astype(BF16)


def scatter_chips(total):
    return lax.psum_scatter(total, "chip", scatter_dimension=0, tiled=False)


def exchange(rows, sign):
    count = lax.axis_size("ep")
    blocks = rows.reshape(count, -1, rows.shape[-1])
    moved = [blocks[0]]
    for d in range(1, count):
        pairs = [(i, (i + sign * d) % count) for i in range(count)]
        moved.append(lax.ppermute(blocks[d], "ep", pairs))
    return jnp.concatenate(moved, axis=0)


def after(value, earlier):
    zero = earlier[(0,) * earlier.ndim].astype(F32) * 0.0
    return value + zero.astype(value.dtype)


def route(ids, experts, capacity):
    micro, rows, _ = ids.shape
    away = lax.rem(ids - lax.axis_index("ep") + experts, experts)
    hits = ids[..., None] == jnp.arange(experts, dtype=jnp.int32)
    per_token = jnp.sum(hits.astype(F32), axis=2)
    earlier = (
        jnp.arange(rows)[:, None] > jnp.arange(rows)[None, :]
    ).astype(BF16)
    before = jnp.einsum(
        "ij,mje->mie", earlier, per_token.astype(BF16), preferred_element_type=F32
    )
    places = jnp.sum(jnp.where(hits, before[:, :, None, :], 0.0), axis=3).astype(jnp.int32)
    step = jnp.arange(micro, dtype=jnp.int32)[:, None, None]
    slots = ((away * micro + step) * capacity + places).reshape(micro * rows, TOP)
    picks = slots[:, :, None] == jnp.arange(experts * micro * capacity, dtype=jnp.int32)
    return hits.reshape(micro * rows, TOP, experts), picks[:, 0], picks[:, 1]


def shards(tokens, expert_ids, router_weight, w_gate, w_up, w_down, cotangent):
    micro, rows, width = tokens.shape
    experts = router_weight.shape[1]
    capacity = min(rows, 3 * rows * TOP // (2 * experts))
    core = lax.axis_index("core")
    gate_w, up_w, down_w = w_gate[0], w_up[0], w_down[0]
    toks = tokens.reshape(micro * rows, width)
    cots = cotangent.reshape(micro * rows, width)

    hits, pick0, pick1 = route(expert_ids, experts, capacity)
    hot0, hot1 = pick0.astype(BF16), pick1.astype(BF16)
    hot = hot0 + hot1

    moved_rows = exchange(contract(hot, toks, 0, 0).astype(BF16), 1)

    partial_logits = contract(router_weight, toks, 0, 1)
    logits = lax.psum(after(partial_logits, moved_rows), ("chip", "core")).T
    chosen = jnp.sum(jnp.where(hits, logits[:, None, :], 0.0), axis=2)
    spread = chosen[:, 0] - chosen[:, 1]
    first = jax.nn.sigmoid(spread)
    second = jax.nn.sigmoid(-spread)
    slot_gate = jnp.sum(
        jnp.where(pick0, first[:, None], 0.0) + jnp.where(pick1, second[:, None], 0.0), axis=0
    )
    sent_cots = (contract(hot, cots, 0, 0) * slot_gate[:, None]).astype(BF16)
    moved_cots = exchange(sent_cots, 1)

    expert_rows = gather_features(moved_rows, core, moved_cots)
    pre_gate = contract(expert_rows, gate_w, 1, 0)
    pre_up = contract(expert_rows, up_w, 1, 0)
    gate_sig = jax.nn.sigmoid(pre_gate)
    gate_act = pre_gate * gate_sig
    hidden = (gate_act * pre_up).astype(BF16)
    keep, send = core_parts(contract(hidden, down_w, 1, 0).astype(BF16), core)
    total = pair_sum(keep, send)
    expert_cots = after(gather_features(moved_cots, core, hidden), total)
    returned = exchange(after(scatter_chips(total), slot_gate), -1)

    hidden_grad = contract(expert_cots, down_w, 1, 1)
    gate_pre_grad = (
        hidden_grad * pre_up * (gate_sig * (1.0 + pre_gate * (1.0 - gate_sig)))
    ).astype(BF16)
    up_pre_grad = (hidden_grad * gate_act).astype(BF16)
    inputs = (contract(gate_pre_grad, gate_w, 1, 1) + contract(up_pre_grad, up_w, 1, 1)).astype(BF16)
    keep_in, send_in = core_parts(inputs, core)
    scattered_in = scatter_chips(pair_sum(keep_in, send_in))

    down_grad = contract(hidden, expert_cots, 0, 0).astype(BF16)
    gate_grad = contract(expert_rows, gate_pre_grad, 0, 0).astype(BF16)
    up_grad = contract(expert_rows, up_pre_grad, 0, 0).astype(BF16)

    first_out = contract(hot0, returned, 1, 0)
    second_out = contract(hot1, returned, 1, 0)
    mixed = (first[:, None] * first_out + second[:, None] * second_out).astype(BF16)
    cot_wide = cots.astype(F32)
    partial_dots = jnp.sum(cot_wide * (first_out - second_out), axis=1)
    partial_dots = after(partial_dots, slot_gate)
    gate_dots = lax.psum(partial_dots, ("chip", "core"))
    delta = gate_dots * first * second
    logit_grad = delta[:, None] * (hits[:, 0].astype(F32) - hits[:, 1].astype(F32))
    router_grad = lax.psum(
        lax.dot_general(
            logit_grad, toks.astype(F32), (((0,), (0,)), ((), ())), precision=lax.Precision.HIGHEST
        ),
        "ep",
    ).T
    router_in = lax.dot_general(
        logit_grad,
        router_weight.astype(F32),
        (((1,), (1,)), ((), ())),
        precision=lax.Precision.HIGHEST,
    )
    returned_grad = exchange(after(scattered_in, router_grad), -1)
    token_grad = (contract(hot, returned_grad, 1, 0) + router_in).astype(BF16)
    return (
        mixed.reshape(tokens.shape),
        token_grad.reshape(tokens.shape),
        gate_grad[None],
        up_grad[None],
        down_grad[None],
        router_grad,
    )


def dot(left, right, left_dim=1, right_dim=0):
    return lax.dot_general(
        left, right, (((left_dim,), (right_dim,)), ((), ())), preferred_element_type=F32
    )


def exact(left, right, left_dim=1, right_dim=0):
    total = None
    for _ in range(3):
        part = left.astype(BF16)
        left = left - part.astype(F32)
        term = dot(part, right, left_dim, right_dim)
        total = term if total is None else total + term
    return total


def layer_kernel(
    micro, ep_size, cap,
    ids_ref, router_ref, toks_ref, cots_ref, wg_hbm, wu_hbm, wd_hbm,
    gate_out, up_out, down_out, mixed_ref, token_grad_ref, router_grad_ref,
    x_buf, c_buf, wg, wu, wd, pg, pu, hid, gpg, upg, hg, stage, total, pair_in, relay_in,
    side_in, out_ret, in_ret, part_ref, hit_ref, slot_ref, gates_ref, logit_grad_ref,
    logit_buf, dots_buf, dots_z, dots_own, router_buf,
    w_sem, z_send, z_recv, ag_send, ag_recv, small_send, small_recv,
    pair_send, pair_recv, rs_send, rs_recv, back_send, back_recv, out_sem, credit,
):
    pieces, slots, width = x_buf.shape
    hidden_width = hid.shape[1]
    rows = slots // micro
    half = rows // 2
    tokens_one = toks_ref.shape[0] // micro
    chip, core, ep = lax.axis_index("chip"), lax.axis_index("core"), lax.axis_index("ep")
    chip_x = chip + 1 - 2 * (chip % 2)
    chip_y = (chip + 2) % SQUARE
    chip_d = SQUARE - 1 - chip
    other = 1 - core
    dev_x, dev_y, dev_pair = (chip_x, core, ep), (chip_y, core, ep), (chip, other, ep)
    me = chip * CORES + core

    def rep_peer(i):
        peer = (me + i) % pieces
        return (peer // CORES, peer % CORES, ep)

    def ep_peer(d):
        return (chip, core, (ep + d + ep_size) % ep_size)

    def remote(source, target, send, recv, device):
        return pltpu.make_async_remote_copy(
            src_ref=source, dst_ref=target, send_sem=send, recv_sem=recv,
            device_id=device, device_id_type=MESH,
        )

    def piece_of(which, kind):
        return which * CORES + kind

    def weight_copy(i):
        if i == 0:
            return pltpu.make_async_copy(wg_hbm, wg, w_sem.at[0])
        if i == 1:
            return pltpu.make_async_copy(wu_hbm, wu, w_sem.at[1])
        return pltpu.make_async_copy(
            wd_hbm.at[:, pl.ds((i - 2) * width, width)], wd.at[i - 2], w_sem.at[i]
        )

    for i in range(2 + pieces):
        weight_copy(i).start()

    barrier = pltpu.get_barrier_semaphore()
    for i in range(1, pieces):
        pl.semaphore_signal(barrier, inc=1, device_id=rep_peer(i), device_id_type=MESH)
    for d in range(1, ep_size):
        pl.semaphore_signal(barrier, inc=1, device_id=ep_peer(d), device_id_type=MESH)

    experts, everyone = router_ref.shape[0], toks_ref.shape[0]
    expert_row = lax.broadcasted_iota(jnp.int32, (experts, everyone), 0)
    hits = [(expert_row == ids_ref[k : k + 1]).astype(F32) for k in range(TOP)]
    hit_ref[...] = hits[0] - hits[1]
    named = hits[0] + hits[1]
    sooner = lax.broadcasted_iota(jnp.int32, (tokens_one, tokens_one), 0)
    later = lax.broadcasted_iota(jnp.int32, (tokens_one, tokens_one), 1)
    earlier = (sooner < later).astype(BF16)
    for m in range(micro):
        span = slice(m * tokens_one, (m + 1) * tokens_one)
        before = dot(named[:, span].astype(BF16), earlier)
        for k in range(TOP):
            place = jnp.sum(hits[k][:, span] * before, axis=0, keepdims=True).astype(jnp.int32)
            ids = ids_ref[k : k + 1, span]
            away = jnp.where(ids >= ep, ids - ep, ids - ep + ep_size)
            slot_ref[k : k + 1, span] = away * cap + place
    part_ref[...] = dot(router_ref[...], toks_ref[...], 1, 1)

    def picks(m):
        span = slice(m * tokens_one, (m + 1) * tokens_one)
        slot_row = lax.broadcasted_iota(jnp.int32, (rows, tokens_one), 0)
        return [(slot_row == slot_ref[k : k + 1, span]).astype(F32) for k in range(TOP)]

    def dispatch(m, source):
        chosen = picks(m)
        hot = (chosen[0] + chosen[1]).astype(BF16)
        return chosen, dot(hot, source[m * tokens_one : (m + 1) * tokens_one])

    def gather_small(source, target, base):
        copies = [
            remote(source, target.at[i], small_send.at[base + i], small_recv.at[base + i], rep_peer(i))
            for i in range(1, pieces)
        ]
        for copy in copies:
            copy.start()
        return copies

    def z_copy(a, m, d):
        source = stage.at[a * micro + m, pl.ds(d * cap, cap)]
        buf = x_buf if a == 0 else c_buf
        target = buf.at[me, pl.ds(m * rows + d * cap, cap)]
        return remote(source, target, z_send.at[a, m, d], z_recv.at[a, m, d], ep_peer(d))

    for m in range(micro):
        value = dispatch(m, toks_ref)[1].astype(BF16)
        stage[m] = value
        x_buf[me, m * rows : m * rows + cap] = value[:cap]
        if m == 0:
            pl.semaphore_wait(barrier, pieces - 1 + ep_size - 1)
            logit_copies = gather_small(part_ref, logit_buf, 0)
        for d in range(1, ep_size):
            z_copy(0, m, d).start()

    for copy in logit_copies:
        copy.wait_recv()
    logits = part_ref[...]
    for i in range(1, pieces):
        logits = logits + logit_buf[i]
    spread = jnp.sum(hit_ref[...] * logits, axis=0, keepdims=True)
    first = jax.nn.sigmoid(spread)
    second = jax.nn.sigmoid(-spread)
    row = lax.broadcasted_iota(jnp.int32, gates_ref.shape, 0)
    gates_ref[...] = jnp.where(row == 0, first, jnp.where(row == 1, second, 0.0))

    for m in range(micro):
        span = slice(m * tokens_one, (m + 1) * tokens_one)
        chosen, value = dispatch(m, cots_ref)
        weight = jnp.sum(
            chosen[0] * first[:, span] + chosen[1] * second[:, span], axis=1, keepdims=True
        )
        scaled = (value * weight).astype(BF16)
        stage[micro + m] = scaled
        c_buf[me, m * rows : m * rows + cap] = scaled[:cap]
        for d in range(1, ep_size):
            z_copy(1, m, d).start()

    def ag_copy(a, m, i):
        buf = x_buf if a == 0 else c_buf
        low, high = pl.ds(m * rows, half), pl.ds(m * rows + half, half)
        full = pl.ds(m * rows, rows)
        piece, span, device = [
            (me, low, dev_x), (me, high, dev_x), (me, high, dev_y), (me, low, dev_y),
            (piece_of(chip_x, core), low, dev_y), (piece_of(chip_y, core), high, dev_x),
            (me, full, dev_pair), (piece_of(chip_x, core), full, dev_pair),
            (piece_of(chip_y, core), full, dev_pair), (piece_of(chip_d, core), full, dev_pair),
        ][i]
        ref = buf.at[piece, span]
        return remote(ref, ref, ag_send.at[a, m, i], ag_recv.at[a, m, i], device)

    def ag_arrive(a, m, i):
        ag_copy(a, m, i).wait_recv()

    def ag_start(a, m):
        for d in range(1, ep_size):
            z_copy(a, m, d).wait_recv()
        for i in (0, 2, 1, 3, 6):
            ag_copy(a, m, i).start()

    def ag_relay(a, m):
        ag_arrive(a, m, 0)
        ag_copy(a, m, 4).start()
        ag_arrive(a, m, 2)
        ag_copy(a, m, 5).start()
        ag_arrive(a, m, 1)
        ag_copy(a, m, 7).start()
        ag_arrive(a, m, 3)
        ag_copy(a, m, 8).start()

    def ag_diag(a, m):
        ag_arrive(a, m, 4)
        ag_arrive(a, m, 5)
        ag_copy(a, m, 9).start()

    order = (chip, chip_x, chip_y, chip_d)
    tile = 512

    def forward(m, s):
        if m == 0 and s == 0:
            weight_copy(0).wait()
            weight_copy(1).wait()
        ag_arrive(0, m, 6 + s)
        which = order[s]

        @pl.loop(0, hidden_width // tile)
        def _(n):
            cols = pl.ds(pl.multiple_of(n * tile, tile), tile)
            span = pl.ds(m * rows, rows)
            one, two = x_buf[piece_of(which, 0), span], x_buf[piece_of(which, 1), span]
            gate = dot(one, wg[piece_of(which, 0), :, cols]) + dot(two, wg[piece_of(which, 1), :, cols])
            up = dot(one, wu[piece_of(which, 0), :, cols]) + dot(two, wu[piece_of(which, 1), :, cols])
            if s == 0:
                pg[span, cols] = gate
                pu[span, cols] = up
            else:
                pg[span, cols] += gate
                pu[span, cols] += up

    strip = 32

    def activate(m):
        @pl.loop(0, rows // strip)
        def _(r):
            span = pl.ds(pl.multiple_of(m * rows + r * strip, strip), strip)
            gate, up = pg[span], pu[span]
            sig = jax.nn.sigmoid(gate)
            act = gate * sig
            hid[span] = (act * up).astype(BF16)
            pu[span] = up * (sig * (1.0 + gate * (1.0 - sig)))
            pg[span] = act

    def backward(m, s):
        ag_arrive(1, m, 6 + s)
        which = order[s]

        @pl.loop(0, hidden_width // tile)
        def _(n):
            cols = pl.ds(pl.multiple_of(n * tile, tile), tile)
            span = pl.ds(m * rows, rows)
            one, two = c_buf[piece_of(which, 0), span], c_buf[piece_of(which, 1), span]
            grad = dot(one, wd[piece_of(which, 0), cols], 1, 1) + dot(two, wd[piece_of(which, 1), cols], 1, 1)
            if s == 0:
                hg[:, cols] = grad
            else:
                hg[:, cols] += grad

    lanes = 128

    def gradients(m):
        @pl.loop(0, rows // strip)
        def _(r):
            span = pl.ds(pl.multiple_of(m * rows + r * strip, strip), strip)
            here = pl.ds(pl.multiple_of(r * strip, strip), strip)
            grad = hg[here]
            gpg[span] = (grad * pu[span]).astype(BF16)
            upg[span] = (grad * pg[span]).astype(BF16)
            both = grad * hid[span].astype(F32)
            part = both[:, :lanes]
            for i in range(1, hidden_width // lanes):
                part = part + both[:, i * lanes : (i + 1) * lanes]
            hg[here, :lanes] = part

        sums = jnp.sum(hg[:, :lanes].T, axis=0, keepdims=True)
        mark = lax.broadcasted_iota(jnp.int32, dots_own.shape, 0) == m
        if m == 0:
            dots_own[...] = jnp.where(mark, sums, 0.0)
        else:
            dots_own[...] = jnp.where(mark, sums, dots_own[...])

    def wait_down():
        for i in range(2, 2 + pieces):
            weight_copy(i).wait()

    def partial(a, m, piece, target):
        span = pl.ds(m * rows, rows)
        if a == 0:
            value = dot(hid[span], wd[piece])
        else:
            value = dot(gpg[span], wg[piece], 1, 1) + dot(upg[span], wu[piece], 1, 1)
        target[...] = value.astype(BF16)

    def rs_chip(j):
        flip = SQUARE - 1 - j
        return (chip // 2 + flip // 2) % 2 * 2 + (chip + flip) % 2

    from_d, from_y, from_x, own = range(SQUARE)

    def pair_copy(a, m, j):
        return remote(
            stage.at[j], pair_in.at[m, j], pair_send.at[a, m, j], pair_recv.at[a, m, j], dev_pair
        )

    low_half, high_half = pl.ds(0, half), pl.ds(half, half)

    def rs_copy(a, m, i):
        source, span, target, device = [
            (from_d, low_half, relay_in.at[m, 0], dev_x),
            (from_d, high_half, relay_in.at[m, 1], dev_y),
            (from_y, high_half, side_in.at[m, 1, high_half], dev_y),
            (from_x, low_half, side_in.at[m, 0, low_half], dev_x),
            (from_y, low_half, side_in.at[m, 1, low_half], dev_y),
            (from_x, high_half, side_in.at[m, 0, high_half], dev_x),
        ][i]
        return remote(
            total.at[m, source, span], target, rs_send.at[a, m, i], rs_recv.at[a, m, i], device
        )

    def back_copy(a, m, d):
        target = out_ret if a == 0 else in_ret
        source = total.at[m, 3, pl.ds(d * cap, cap)]
        return remote(
            source, target.at[m, pl.ds(d * cap, cap)], back_send.at[a, m, d], back_recv.at[a, m, d], ep_peer(-d)
        )

    def scatter_pair(a, m):
        if (a, m) == (0, 0):
            for b in range(2):
                for n in range(micro):
                    for d in range(1, ep_size):
                        z_copy(b, n, d).wait_send()
        else:
            before = (a, m - 1) if m > 0 else (a - 1, micro - 1)
            for j in range(SQUARE):
                pair_copy(before[0], before[1], j).wait_send()
        if a == 1:
            pl.semaphore_wait(credit.at[m], 3)

        @pl.loop(0, SQUARE)
        def _(j):
            partial(a, m, piece_of(rs_chip(j), other), stage.at[j])
            pair_copy(a, m, j).start()

        if a == 1:
            for i in range(6):
                rs_copy(0, m, i).wait_send()
            for d in range(1, ep_size):
                back_copy(0, m, d).wait_send()

        @pl.loop(0, SQUARE)
        def _(j):
            partial(a, m, piece_of(rs_chip(j), core), total.at[m, j])

    def add_into(m, j, start, count, others):
        @pl.loop(0, count // strip)
        def _(r):
            span = pl.ds(pl.multiple_of(start + r * strip, strip), strip)
            here = pl.ds(pl.multiple_of(r * strip, strip), strip)
            value = total[m, j, span].astype(F32)
            for ref in others:
                value = value + ref[here].astype(F32)
            total[m, j, span] = value.astype(BF16)

    def scatter_sum(a, m):
        for j in range(SQUARE):
            pair_copy(a, m, j).wait_recv()
            add_into(m, j, 0, rows, (pair_in.at[m, j],))
            if j == 0:
                rs_copy(a, m, 0).start()
                rs_copy(a, m, 1).start()
            elif j < 3:
                rs_copy(a, m, 1 + j).start()

    def scatter_relay(a, m):
        rs_copy(a, m, 0).wait_recv()
        add_into(m, from_y, 0, half, (relay_in.at[m, 0],))
        rs_copy(a, m, 4).start()
        rs_copy(a, m, 1).wait_recv()
        add_into(m, from_x, half, half, (relay_in.at[m, 1],))
        rs_copy(a, m, 5).start()

    def scatter_last(a, m):
        for i in (2, 3, 4, 5):
            rs_copy(a, m, i).wait_recv()
        add_into(m, 3, 0, rows, (side_in.at[m, 0], side_in.at[m, 1]))
        for d in range(1, ep_size):
            back_copy(a, m, d).start()
        (out_ret if a == 0 else in_ret)[m, 0:cap] = total[m, 3, 0:cap]
        if a == 0:
            for device in (dev_pair, dev_x, dev_y):
                pl.semaphore_signal(credit.at[m], inc=1, device_id=device, device_id_type=MESH)

    def out_copy(kind, piece):
        if kind == 0:
            return pltpu.make_async_copy(
                wd.at[piece], down_out.at[:, pl.ds(piece * width, width)], out_sem.at[0, piece]
            )
        if kind == 1:
            return pltpu.make_async_copy(wg.at[piece], gate_out.at[piece], out_sem.at[1, piece])
        return pltpu.make_async_copy(wu.at[piece], up_out.at[piece], out_sem.at[2, piece])

    def weight_grads(kind, start, stop):
        @pl.loop(start, stop)
        def _(piece):
            if kind == 0:
                @pl.loop(0, hidden_width // tile)
                def _(n):
                    cols = pl.ds(pl.multiple_of(n * tile, tile), tile)
                    wd[piece, cols] = dot(hid[:, cols], c_buf[piece], 0, 0).astype(BF16)
            else:
                grad, keep = (gpg, wg) if kind == 1 else (upg, wu)
                keep[piece] = dot(x_buf[piece], grad[...], 0, 0).astype(BF16)
            out_copy(kind, piece).start()

    def mix(m):
        for d in range(1, ep_size):
            back_copy(0, m, d).wait_recv()
        span = slice(m * tokens_one, (m + 1) * tokens_one)
        chosen = picks(m)
        weight = chosen[0] * gates_ref[0:1, span] + chosen[1] * gates_ref[1:2, span]
        mixed_ref[span] = exact(weight, out_ret[m], 0, 0).astype(BF16)

    def collect(m):
        for d in range(1, ep_size):
            back_copy(1, m, d).wait_recv()
        span = slice(m * tokens_one, (m + 1) * tokens_one)
        chosen = picks(m)
        hot = (chosen[0] + chosen[1]).astype(BF16)
        value = dot(hot, in_ret[m], 0, 0)
        value = value + exact(logit_grad_ref[:, span], router_ref[...], 0, 0)
        token_grad_ref[span] = value.astype(BF16)

    ag_start(0, 0)
    forward(0, 0)
    ag_relay(0, 0)
    forward(0, 1)
    ag_start(0, 1)
    forward(0, 2)
    ag_diag(0, 0)
    forward(1, 0)
    forward(0, 3)
    activate(0)
    ag_relay(0, 1)
    ag_start(1, 0)
    wait_down()
    scatter_pair(0, 0)
    ag_diag(0, 1)
    forward(1, 1)
    forward(1, 2)
    ag_relay(1, 0)
    scatter_sum(0, 0)
    forward(1, 3)
    activate(1)
    scatter_pair(0, 1)
    ag_diag(1, 0)
    scatter_relay(0, 0)
    ag_start(1, 1)
    for s in range(4):
        backward(0, s)
    gradients(0)
    scatter_last(0, 0)
    scatter_pair(1, 0)
    ag_relay(1, 1)
    scatter_sum(0, 1)
    for s in range(3):
        backward(1, s)
    ag_diag(1, 1)
    backward(1, 3)
    gradients(1)
    dots_copies = gather_small(dots_own, dots_buf, pieces)
    scatter_relay(0, 1)
    scatter_sum(1, 0)
    weight_grads(0, 0, pieces // 2)
    scatter_last(0, 1)
    for copy in dots_copies:
        copy.wait_recv()
    dots = dots_own[...]
    for i in range(1, pieces):
        dots = dots + dots_buf[i]
    dots_z[0] = dots
    dots_back = [
        remote(dots_z.at[0], dots_z.at[d], small_send.at[2 * pieces + d], small_recv.at[2 * pieces + d], ep_peer(-d))
        for d in range(1, ep_size)
    ]
    for copy in dots_back:
        copy.start()
    scatter_pair(1, 1)
    scatter_relay(1, 0)
    scatter_sum(1, 1)
    weight_grads(0, pieces // 2, pieces)
    scatter_last(1, 0)
    for copy in dots_back:
        copy.wait_recv()
    owner = lax.broadcasted_iota(jnp.int32, dots_own.shape, 1) // cap
    mine = jnp.where(owner == 0, dots_z[0], 0.0)
    for d in range(1, ep_size):
        mine = jnp.where(owner == d, dots_z[d], mine)
    for m in range(micro):
        span = slice(m * tokens_one, (m + 1) * tokens_one)
        chosen = picks(m)
        zero = exact(mine, chosen[0].astype(BF16))[m : m + 1]
        one = exact(mine, chosen[1].astype(BF16))[m : m + 1]
        delta = gates_ref[1:2, span] * zero - gates_ref[0:1, span] * one
        logit_grad_ref[:, span] = delta * hit_ref[:, span]
    router_buf[0] = exact(logit_grad_ref[...], toks_ref[...])
    router_copies = [
        remote(router_buf.at[0], router_buf.at[d], small_send.at[2 * pieces + ep_size + d], small_recv.at[2 * pieces + ep_size + d], ep_peer(d))
        for d in range(1, ep_size)
    ]
    for copy in router_copies:
        copy.start()
    weight_grads(1, 0, pieces // 2)
    scatter_relay(1, 1)
    weight_grads(1, pieces // 2, pieces)
    mix(0)
    mix(1)
    scatter_last(1, 1)
    weight_grads(2, 0, pieces)
    for copy in router_copies:
        copy.wait_recv()
    router = router_buf[0]
    for d in range(1, ep_size):
        router = router + router_buf[d]
    router_grad_ref[...] = router
    for m in range(micro):
        collect(m)

    for a in range(2):
        for m in range(micro):
            for d in range(1, ep_size):
                if a == 1:
                    back_copy(a, m, d).wait_send()
            for i in range(10):
                ag_copy(a, m, i).wait_send()
            if a == 1:
                for i in range(6):
                    rs_copy(a, m, i).wait_send()
    for j in range(SQUARE):
        pair_copy(1, micro - 1, j).wait_send()
    for copy in logit_copies + dots_copies + dots_back + router_copies:
        copy.wait_send()
    for kind in range(3):
        for piece in range(pieces):
            out_copy(kind, piece).wait()


def square_shards(tokens, expert_ids, router_weight, w_gate, w_up, w_down, cotangent):
    micro, rows, width = tokens.shape
    experts = router_weight.shape[1]
    capacity = min(rows, 3 * rows * TOP // (2 * experts))
    ep_size = lax.axis_size("ep")
    pieces = lax.axis_size("chip") * CORES
    count = experts * capacity
    slots = micro * count
    hidden_width = w_down.shape[1]
    sub = max(8, -(-experts // 8) * 8)
    toks = tokens.reshape(micro * rows, width)
    cots = cotangent.reshape(micro * rows, width)
    ids = jnp.moveaxis(expert_ids, -1, 0).reshape(TOP, micro * rows)
    router_rows = jnp.pad(router_weight.T, ((0, sub - experts), (0, 0)))

    vmem = pl.BlockSpec(memory_space=pltpu.VMEM)
    hbm = pl.BlockSpec(memory_space=pl.ANY)
    shape = jax.ShapeDtypeStruct
    dma = pltpu.SemaphoreType.DMA
    features = w_gate.shape[1]
    wide = shape((pieces, width, hidden_width), BF16)
    half = count // 2
    sizes = dict(collective_id=0, has_side_effects=True, vmem_limit_bytes=VMEM_BYTES)
    gate_grad, up_grad, down_grad, mixed, token_grad, router = pl.pallas_call(
        functools.partial(layer_kernel, micro, ep_size, capacity),
        out_shape=(
            wide, wide, shape((hidden_width, features), BF16),
            shape(toks.shape, BF16), shape(toks.shape, BF16), shape((sub, width), F32),
        ),
        in_specs=[vmem] * 4 + [hbm] * 3,
        out_specs=(hbm,) * 3 + (vmem,) * 3,
        scratch_shapes=[
            pltpu.VMEM((pieces, slots, width), BF16),
            pltpu.VMEM((pieces, slots, width), BF16),
            pltpu.VMEM((pieces, width, hidden_width), BF16),
            pltpu.VMEM((pieces, width, hidden_width), BF16),
            pltpu.VMEM((pieces, hidden_width, width), BF16),
            pltpu.VMEM((slots, hidden_width), F32),
            pltpu.VMEM((slots, hidden_width), F32),
            pltpu.VMEM((slots, hidden_width), BF16),
            pltpu.VMEM((slots, hidden_width), BF16),
            pltpu.VMEM((slots, hidden_width), BF16),
            pltpu.VMEM((count, hidden_width), F32),
            pltpu.VMEM((max(SQUARE, 2 * micro), count, width), BF16),
            pltpu.VMEM((micro, SQUARE, count, width), BF16),
            pltpu.VMEM((micro, SQUARE, count, width), BF16),
            pltpu.VMEM((micro, 2, half, width), BF16),
            pltpu.VMEM((micro, 2, count, width), BF16),
            pltpu.VMEM((micro, count, width), BF16),
            pltpu.VMEM((micro, count, width), BF16),
            pltpu.VMEM((sub, micro * rows), F32),
            pltpu.VMEM((sub, micro * rows), F32),
            pltpu.VMEM((TOP, micro * rows), jnp.int32),
            pltpu.VMEM((sub, micro * rows), F32),
            pltpu.VMEM((sub, micro * rows), F32),
            pltpu.VMEM((pieces, sub, micro * rows), F32),
            pltpu.VMEM((pieces, 8, count), F32),
            pltpu.VMEM((ep_size, 8, count), F32),
            pltpu.VMEM((8, count), F32),
            pltpu.VMEM((ep_size, sub, width), F32),
            dma((2 + pieces,)),
            dma((2, micro, ep_size)),
            dma((2, micro, ep_size)),
            dma((2, micro, 10)),
            dma((2, micro, 10)),
            dma((2 * pieces + 2 * ep_size,)),
            dma((2 * pieces + 2 * ep_size,)),
            dma((2, micro, SQUARE)),
            dma((2, micro, SQUARE)),
            dma((2, micro, 6)),
            dma((2, micro, 6)),
            dma((2, micro, ep_size)),
            dma((2, micro, ep_size)),
            dma((3, pieces)),
            pltpu.SemaphoreType.REGULAR((micro,)),
        ],
        compiler_params=pltpu.CompilerParams(**sizes),
    )(
        ids, router_rows, toks, cots,
        w_gate.reshape(pieces, width, hidden_width),
        w_up.reshape(pieces, width, hidden_width),
        w_down[0],
    )
    return (
        mixed.reshape(tokens.shape),
        token_grad.reshape(tokens.shape),
        gate_grad.reshape(w_gate.shape),
        up_grad.reshape(w_up.shape),
        down_grad[None],
        router[:experts].T,
    )


def solution(mesh):
    rep, ep = mesh.shape["rep"], mesh.shape["ep"]
    inner = Mesh(mesh.devices.reshape(rep // CORES, CORES, ep), ("chip", "core", "ep"))
    reps = ("chip", "core")
    in_specs = (
        P(None, "ep", reps),
        P(None, "ep", None),
        P(reps, None),
        P("ep", None, reps),
        P("ep", None, reps),
        P("ep", reps, None),
        P(None, "ep", reps),
    )
    out_specs = (
        P(None, "ep", reps),
        P(None, "ep", reps),
        P("ep", None, reps),
        P("ep", None, reps),
        P("ep", reps, None),
        P(reps, None),
    )
    body = square_shards if rep // CORES == SQUARE else shards
    return jax.shard_map(body, mesh=inner, in_specs=in_specs, out_specs=out_specs, check_vma=False)
```
